32 devices in a mesh: tile: 8 (over z, x), conv: 4 (over y, core).
Axes of the slice: x: 2, y: 2, z: 4, core: 2. Of those that a mesh axis runs over, the one named last changes fastest.
Arguments:
- field: float32 [256, 24576], P(None, ('tile', 'conv')), may hold values from -6 to 6
- interp: bfloat16 [32768, 384], P(('tile', 'conv')), may hold values from -0.1875 to 0.1875
- conv_blocks: bfloat16 [64, 3, 256, 256], P(('tile', 'conv')), may hold values from -0.21875 to 0.21875
- band_shift: int32 [64, 3], P(('tile', 'conv')), may hold values from 0 to 1
- owner: int32 [12288, 1], P(('tile', 'conv')), may hold values from 0 to 3; in each aligned block of 384 rows (0 to 383, 384 to 767, ...) at most 128 rows name the same one
- edge_index: int32 [64, 128], P(('tile', 'conv')), may hold values from 0 to 767, as said below
Outputs:
- correlated: float32 [256, 24576], P(None, ('tile', 'conv'))
The draws below stay inside these ranges and needn't reach their ends.
Inputs may be any that keep to these rules, and one draw needn't show every extreme that they name: `edge_index`: row 2b lists the first 128 columns of domain b in some order, row 2b + 1 its last 128 columns in some order. Among the 384 points of one domain no owner is named more than 128 times, and in some domains one owner is named exactly 128 times.
All inputs are finite; a program needn't handle non-finite values.
Results may differ from the reference program's by a relative error of at most 0.0049.
Values may be sent and summed in bfloat16 or wider, within the bound.
A program may use at most 64 MiB of HBM per device.

```python
import math
import jax
import jax.numpy as jnp
import numpy as np
from jax import lax

COLUMNS = 768
HALO_WIDTH = 128
BLOCK_POINTS = 256
OWNER_BLOCKS = 2
BAND_COUNT = 3
FIELD_ROWS = 256
DOMAINS = 32
ALL_COLUMNS = 24576
EXTENDED = 1024
SLOTS = 512
SUBPOINTS = 384
CAPACITY = 128
ALL_SUBPOINTS = 12288
N_TILE = 8
N_CONV = 4


def draw_edge_index(key, part):
    row_keys = jax.random.split(key, 2 * DOMAINS)
    orders = jax.vmap(lambda single: jax.random.permutation(single, HALO_WIDTH))(row_keys)
    side_flags = jnp.arange(2 * DOMAINS, dtype=jnp.int32) % 2
    offsets = side_flags * (COLUMNS - HALO_WIDTH)
    return (orders.astype(jnp.int32) + offsets[:, None]).astype(jnp.int32)


def with_ends(values, own_key, smallest, high):
    longest = values.shape.index(max(values.shape))
    spots = []
    for shift in (0, 1):
        where = [jax.random.randint(jax.random.fold_in(own_key, axis), (), 0, length) for axis, length in enumerate(values.shape)]
        where[longest] = (where[longest] + shift) % values.shape[longest]
        spots.append(tuple(where))
    return values.at[spots[0]].set(smallest).at[spots[1]].set(high)


def steps_of(key, shape, cuts, low, top_value):
    gain, own = 1.0, jax.random.fold_in(key, 6)
    for axis_at, shards_of in cuts:
        steps = jnp.exp(jax.random.uniform(jax.random.fold_in(own, axis_at), (shards_of,), jnp.float32, low / len(cuts), top_value / len(cuts)))
        gain = gain * jnp.repeat(steps, shape[axis_at] // shards_of).reshape([-1 if axis == axis_at else 1 for axis in range(len(shape))])
    return gain


def routed_block(own_key, own, number, rows, amount, top, limit, skew):
    sequence = jax.random.permutation(own_key, amount)
    crowded, ordinary = portions_of(amount, rows * top, limit, skew, True), portions_of(amount, rows * top, limit, skew, False)
    places = jnp.arange(amount)

    def named(sizes, rotation):
        used = int((sizes > 0).sum())
        fixed = max(1, used // 4)
        passed = fixed + (places - fixed + rotation * (used - fixed)) % max(1, amount - fixed)
        return jnp.zeros((amount,), jnp.int32).at[sequence[jnp.where(places < fixed, places, passed)]].set(jnp.asarray(sizes, jnp.int32))

    sizes = jnp.where(number % 4 == 0, named(crowded, number // 4), named(ordinary, number - number // 4 - 1))
    mixed = jax.random.permutation(jax.random.fold_in(own, 3), amount)
    source_of, taker = mixed[0:amount // 2 * 2:2], mixed[1:amount // 2 * 2:2]
    room = jnp.minimum(sizes[source_of] - 1, limit - sizes[taker]) // 2
    room = jnp.where((source_of == sequence[0]) | (taker == sequence[0]) | (sizes[taker] == 0), 0, jnp.maximum(room, 0))
    passed = jax.random.randint(jax.random.fold_in(own, 4), (amount // 2,), 0, 1 << 20) % (room + 1)
    sizes = sizes.at[source_of].add(-passed).at[taker].add(passed)
    members = jnp.searchsorted(jnp.cumsum(sizes), jnp.arange(rows * top), side="right").astype(jnp.int32)
    listing = members.reshape(top, rows).T
    listing = listing[jax.random.permutation(jax.random.fold_in(own, 1), rows)]
    rotation = jax.random.randint(jax.random.fold_in(own, 2), (rows, 1), 0, top)
    return jnp.take_along_axis(listing, (jnp.arange(top)[None, :] + rotation) % top, axis=1)


def portions_of(count, total, reach, slope, full):
    loads = [(1 << 20) // math.isqrt(grade ** slope) + 1 for grade in range(1, count + 1)]
    largest = reach if full else min(reach, max(-(-total // count), total * loads[0] // sum(loads)))
    least = 1 if total - largest >= count - 1 else 0
    holding, surplus = [largest] + [least] * (count - 1), total - largest - least * (count - 1)
    while surplus > 0:
        movable = [i for i in range(1, count) if holding[i] < largest] or [i for i in range(1, count) if holding[i] < reach]
        mass, remaining = sum([loads[i] for i in movable]), surplus
        for i in movable:
            addition = min(reach - holding[i], max(1, remaining * loads[i] // mass), surplus)
            holding[i] = holding[i] + addition
            surplus = surplus - addition
    return np.array(holding)


def gaussian(stream_key, dims, width, limit, cuts=(), kind=jnp.bfloat16):
    drawn = width * jax.random.normal(stream_key, dims, jnp.float32)
    if cuts:
        drawn = drawn * steps_of(stream_key, dims, cuts, -0.22, 0.18)
    return jnp.clip(drawn, -limit, limit).astype(kind)


def setup_inputs(seed: int = 0) -> dict:
    streams_of = jax.random.split(jax.random.key(seed), 7)
    field = gaussian(streams_of[0], (FIELD_ROWS, ALL_COLUMNS), 1.0, 6.0, ((1, 32),), jnp.float32)
    interp = gaussian(streams_of[1], (DOMAINS * EXTENDED, SUBPOINTS), EXTENDED ** -0.5, 0.1875, ((0, 32),))
    conv_blocks = gaussian(streams_of[2], (DOMAINS * OWNER_BLOCKS, BAND_COUNT, BLOCK_POINTS, BLOCK_POINTS), (BAND_COUNT * BLOCK_POINTS) ** -0.5, 0.21875, ((0, 32),))
    band_shift = with_ends(jax.random.randint(streams_of[3], (DOMAINS * OWNER_BLOCKS, BAND_COUNT), 0, OWNER_BLOCKS), jax.random.fold_in(streams_of[3], 1), 0, OWNER_BLOCKS - 1).astype(jnp.int32)
    owner_keys = jax.random.split(jax.random.fold_in(streams_of[4], 1), ALL_SUBPOINTS // SUBPOINTS)
    owner_turns = jax.random.permutation(jax.random.fold_in(streams_of[4], 3), ALL_SUBPOINTS // SUBPOINTS)
    owner = jax.vmap(lambda own, number: routed_block(jax.random.fold_in(streams_of[4], 2), own, number, SUBPOINTS, N_CONV, 1, CAPACITY, 2))(owner_keys, owner_turns).reshape((ALL_SUBPOINTS, 1))
    edge_index = draw_edge_index(jax.random.fold_in(streams_of[6], 71), 0)
    return dict(field=field, interp=interp, conv_blocks=conv_blocks, band_shift=band_shift, owner=owner, edge_index=edge_index)


def slot_table(owners):
    choose = (owners[:, None] == jnp.arange(N_CONV, dtype=jnp.int32)[None, :]).astype(jnp.int32)
    before = jnp.cumsum(choose, axis=0) - choose
    position = jnp.sum(before * choose, axis=1)
    slot_index = owners * CAPACITY + position
    return (slot_index[:, None] == jnp.arange(SLOTS, dtype=jnp.int32)[None, :]).astype(jnp.float32)


def interpolate(operands):
    extended, weights, owners = operands
    subgrid = jnp.dot(extended, weights, preferred_element_type=jnp.float32).astype(jnp.bfloat16)
    packed = jnp.dot(subgrid.astype(jnp.float32), slot_table(owners), precision=lax.Precision.HIGHEST)
    return packed.astype(jnp.bfloat16)


def convolve(operands):
    values, blocks, shifts = operands
    height = values.shape[0]
    pieces = values.reshape(height, OWNER_BLOCKS, BLOCK_POINTS).astype(jnp.float32)
    source = (jnp.arange(OWNER_BLOCKS, dtype=jnp.int32)[:, None] + shifts) % OWNER_BLOCKS
    picked = pieces[:, source, :]
    matrices = blocks.astype(jnp.float32)
    forward = jnp.einsum("rjbp,jbpq->rjq", picked, matrices, precision=lax.Precision.HIGHEST).astype(jnp.bfloat16)
    backward = jnp.einsum("rjq,jbpq->rjbp", forward.astype(jnp.float32), matrices, precision=lax.Precision.HIGHEST)
    select = (source[:, :, None] == jnp.arange(OWNER_BLOCKS, dtype=jnp.int32)[None, None, :]).astype(jnp.float32)
    adjoint = jnp.einsum("rjbp,jbs->rsp", backward, select, precision=lax.Precision.HIGHEST)
    return adjoint.reshape(height, SLOTS).astype(jnp.bfloat16)


def adjoint_interpolate(operands):
    returned_slots, weights, owners = operands
    returned = jnp.dot(returned_slots.astype(jnp.float32), slot_table(owners).T, precision=lax.Precision.HIGHEST)
    returned = returned.astype(jnp.bfloat16)
    return jnp.dot(returned, weights.T, preferred_element_type=jnp.float32)


def add_edges(inner_part, left_sum, right_sum, left_list, right_list):
    inner_part = inner_part.at[:, left_list].add(left_sum)
    return inner_part.at[:, right_list].add(right_sum)


def reference(field, interp, conv_blocks, band_shift, owner, edge_index):
    field_rows = field.shape[0]
    rounded = field.astype(jnp.bfloat16).reshape(field_rows, DOMAINS, COLUMNS).transpose(1, 0, 2)
    edges = edge_index.reshape(DOMAINS, 2, HALO_WIDTH)
    left_lists = edges[:, 0, :]
    right_lists = edges[:, 1, :]
    left_index = jnp.broadcast_to(left_lists[:, None, :], (DOMAINS, field_rows, HALO_WIDTH))
    right_index = jnp.broadcast_to(right_lists[:, None, :], (DOMAINS, field_rows, HALO_WIDTH))
    left_values = jnp.take_along_axis(rounded, left_index, axis=2)
    right_values = jnp.take_along_axis(rounded, right_index, axis=2)
    extended = jnp.concatenate([jnp.roll(right_values, 1, axis=0), rounded, jnp.roll(left_values, -1, axis=0)], axis=2)
    weights = interp.reshape(DOMAINS, EXTENDED, SUBPOINTS)
    owners = owner.reshape(DOMAINS, SUBPOINTS)
    packed = lax.map(interpolate, (extended, weights, owners))
    gathered = packed.reshape(N_TILE, N_CONV, field_rows, N_CONV, CAPACITY).transpose(0, 3, 2, 1, 4)
    gathered = gathered.reshape(DOMAINS, field_rows, SLOTS)
    blocks = conv_blocks.reshape(DOMAINS, OWNER_BLOCKS, BAND_COUNT, BLOCK_POINTS, BLOCK_POINTS)
    shifts = band_shift.reshape(DOMAINS, OWNER_BLOCKS, BAND_COUNT)
    adjoints = lax.map(convolve, (gathered, blocks, shifts))
    returned = adjoints.reshape(N_TILE, N_CONV, field_rows, N_CONV, CAPACITY).transpose(0, 3, 2, 1, 4)
    returned = returned.reshape(DOMAINS, field_rows, SLOTS)
    partial_value = lax.map(adjoint_interpolate, (returned, weights, owners))
    interior = partial_value[:, :, HALO_WIDTH:HALO_WIDTH + COLUMNS]
    left_sums = jnp.roll(partial_value[:, :, HALO_WIDTH + COLUMNS:], 1, axis=0)
    right_sums = jnp.roll(partial_value[:, :, :HALO_WIDTH], -1, axis=0)
    result = jax.vmap(add_edges)(interior, left_sums, right_sums, left_lists, right_lists)
    return result.transpose(1, 0, 2).reshape(field_rows, DOMAINS * COLUMNS)
```

```python
import functools

import jax
import jax.numpy as jnp
from jax import lax
from jax.experimental import pallas as pl
from jax.experimental.pallas import tpu as pltpu
from jax.sharding import PartitionSpec as P

MESH = pl.DeviceIdType.MESH
CHUNKS = 1


def mm(left, right):
    return lax.dot_general(left, right, (((1,), (0,)), ((), ())), preferred_element_type=jnp.float32)


def mm_t(left, right):
    return lax.dot_general(left, right, (((1,), (1,)), ((), ())), preferred_element_type=jnp.float32)


def kernel(
    tiles, groups, field_hbm, interp_hbm, blocks_hbm, shift_ref, owner_hbm, edge_hbm, out_hbm,
    field, interp, blocks, owner, edge, ip, conv, gram, base, result,
    edge_out, edge_in, slot_out, slot_in, back_out, back_in, part_out, part_in,
    load_sem, store_sem, edge_send, edge_recv, slot_send, slot_recv, back_send, back_recv,
    part_send, part_recv,
):
    rows, columns = field.shape
    extended, points = interp.shape
    rim = edge.shape[1]
    owned, bands, size = blocks.shape[0], blocks.shape[1], blocks.shape[2]
    slots = owned * size
    capacity = slots // groups
    height = rows // CHUNKS
    tile, me = lax.axis_index("tile"), lax.axis_index("conv")
    count = tiles * groups
    place = tile * groups + me
    after, before = lax.rem(place + 1, count), lax.rem(place + count - 1, count)
    right = (lax.div(after, groups), lax.rem(after, groups))
    left = (lax.div(before, groups), lax.rem(before, groups))
    hops = [groups // 2] + [k for k in range(1, groups) if k != groups // 2]
    peers = [lax.rem(me + k, groups) for k in hops]

    barrier = pltpu.get_barrier_semaphore()
    for other in [left, right] + [(tile, peer) for peer in peers]:
        pl.semaphore_signal(barrier, inc=1, device_id=other, device_id_type=MESH)

    def load(source, target, index):
        copy = pltpu.make_async_copy(source, target, load_sem.at[index])
        copy.start()
        return copy

    inner = slice(rim, columns - rim)
    lead, tail = slice(0, rim), slice(columns - rim, columns)
    load_edge = load(edge_hbm, edge, 0)
    load_lead = load(field_hbm.at[:, lead], field.at[:, lead], 1)
    load_tail = load(field_hbm.at[:, tail], field.at[:, tail], 2)
    load_owner = load(owner_hbm, owner, 3)
    load_interp = load(interp_hbm, interp, 4)
    load_inner = load(field_hbm.at[:, inner], field.at[:, inner], 5)
    load_blocks = load(blocks_hbm, blocks, 6)

    def piece(chunk):
        return slice(chunk * height, (chunk + 1) * height)

    def pair(send, recv, out_ref, in_ref, chunk, side, target):
        return pltpu.make_async_remote_copy(
            src_ref=out_ref.at[chunk, side], dst_ref=in_ref.at[chunk, side],
            send_sem=send.at[chunk, side], recv_sem=recv.at[chunk, side],
            device_id=target, device_id_type=MESH,
        )

    def exchange(send, recv, out_ref, in_ref, chunk):
        copies = []
        for peer in peers:
            copies.append(pltpu.make_async_remote_copy(
                src_ref=out_ref.at[chunk, peer], dst_ref=in_ref.at[chunk, me],
                send_sem=send.at[chunk, peer], recv_sem=recv.at[chunk, me],
                device_id=(tile, peer), device_id_type=MESH,
            ))
            copies[-1].start()
        in_ref[chunk, me] = out_ref[chunk, me]
        return copies

    def arrived(send, recv, out_ref, in_ref, chunk):
        for peer in peers:
            pltpu.make_async_remote_copy(
                src_ref=out_ref.at[chunk, peer], dst_ref=in_ref.at[chunk, peer],
                send_sem=send.at[chunk, peer], recv_sem=recv.at[chunk, peer],
                device_id=(tile, peer), device_id_type=MESH,
            ).wait_recv()
        return jnp.concatenate([in_ref[chunk, g] for g in range(groups)], axis=1)

    load_edge.wait()
    lines = lax.broadcasted_iota(jnp.int32, (rim, rim), 0)
    left_pick = (lines == edge[0:1, :]).astype(jnp.float32).astype(jnp.bfloat16)
    right_pick = (lines + (columns - rim) == edge[1:2, :]).astype(jnp.float32).astype(jnp.bfloat16)
    load_lead.wait()
    load_tail.wait()
    for chunk in range(CHUNKS):
        part = piece(chunk)
        edge_out[chunk, 0] = mm(field[part, tail].astype(jnp.bfloat16), right_pick).astype(jnp.bfloat16)
        edge_out[chunk, 1] = mm(field[part, lead].astype(jnp.bfloat16), left_pick).astype(jnp.bfloat16)
    pl.semaphore_wait(barrier, 2 + len(peers))
    edge_copies, part_copies, slot_copies, back_copies = [], [], [], []
    for chunk in range(CHUNKS):
        for side, target in ((0, right), (1, left)):
            copy = pair(edge_send, edge_recv, edge_out, edge_in, chunk, side, target)
            copy.start()
            edge_copies.append(copy)

    load_owner.wait()
    owners = owner[...]
    choose = (owners == lax.broadcasted_iota(jnp.int32, (-(-groups // 8) * 8, points), 0)).astype(jnp.float32)
    order = lax.broadcasted_iota(jnp.int32, (points, points), 0) < lax.broadcasted_iota(
        jnp.int32, (points, points), 1
    )
    ranks = mm(choose.astype(jnp.bfloat16), order.astype(jnp.float32).astype(jnp.bfloat16))
    rank = jnp.sum(ranks * choose, axis=0, keepdims=True)
    slot = owners * capacity + rank.astype(jnp.int32)
    placement = (slot == lax.broadcasted_iota(jnp.int32, (slots, points), 0)).astype(jnp.float32)
    placement = placement.astype(jnp.bfloat16)
    load_interp.wait()
    ip[0:rim, :] = mm_t(interp[0:rim, :], placement).astype(jnp.bfloat16)
    ip[rim : 2 * rim, :] = mm_t(interp[extended - rim :, :], placement).astype(jnp.bfloat16)
    ip[2 * rim :, :] = mm_t(interp[rim : extended - rim, :], placement).astype(jnp.bfloat16)
    load_inner.wait()
    base[...] = mm(field[...].astype(jnp.bfloat16), ip[2 * rim :, :])

    load_blocks.wait()
    for j in range(owned):
        for s in range(owned):
            total = jnp.zeros((size, size), jnp.float32)
            for c in range(bands):
                reads = lax.rem(j + shift_ref[j, c], owned) == s
                total = total + jnp.where(reads, 1.0, 0.0) * blocks[j, c].astype(jnp.float32)
            conv[s * size : (s + 1) * size, j * size : (j + 1) * size] = total.astype(jnp.bfloat16)
    gram[...] = mm_t(conv[...], conv[...]).astype(jnp.bfloat16)

    for chunk in range(CHUNKS):
        for side, target in ((0, right), (1, left)):
            pair(edge_send, edge_recv, edge_out, edge_in, chunk, side, target).wait_recv()
        edges = jnp.concatenate([edge_in[chunk, 0], edge_in[chunk, 1]], axis=1)
        subgrid = (base[piece(chunk), :] + mm(edges, ip[0 : 2 * rim, :])).astype(jnp.bfloat16)
        for g in range(groups):
            slot_out[chunk, g] = subgrid[:, g * capacity : (g + 1) * capacity]
        slot_copies += exchange(slot_send, slot_recv, slot_out, slot_in, chunk)

    for chunk in range(CHUNKS):
        gathered = arrived(slot_send, slot_recv, slot_out, slot_in, chunk)
        adjoint = mm(gathered, gram[...]).astype(jnp.bfloat16)
        for g in range(groups):
            back_out[chunk, g] = adjoint[:, g * capacity : (g + 1) * capacity]
        back_copies += exchange(back_send, back_recv, back_out, back_in, chunk)

    stores = []
    for chunk in range(CHUNKS):
        part = piece(chunk)
        returned = arrived(back_send, back_recv, back_out, back_in, chunk)
        rims = mm_t(returned, ip[0 : 2 * rim, :]).astype(jnp.bfloat16)
        part_out[chunk, 0] = rims[:, rim:]
        part_out[chunk, 1] = rims[:, :rim]
        for side, target in ((0, right), (1, left)):
            copy = pair(part_send, part_recv, part_out, part_in, chunk, side, target)
            copy.start()
            part_copies.append(copy)
        result[part, :] = mm_t(returned, ip[2 * rim :, :])
        copy = pltpu.make_async_copy(
            result.at[part, inner], out_hbm.at[part, inner], store_sem.at[chunk, 0]
        )
        copy.start()
        stores.append(copy)

    for chunk in range(CHUNKS):
        part = piece(chunk)
        for side, where, pick, target in ((0, lead, left_pick, right), (1, tail, right_pick, left)):
            pair(part_send, part_recv, part_out, part_in, chunk, side, target).wait_recv()
            result[part, where] += mm_t(part_in[chunk, side], pick)
            copy = pltpu.make_async_copy(
                result.at[part, where], out_hbm.at[part, where], store_sem.at[chunk, 1 + side]
            )
            copy.start()
            stores.append(copy)
    for copy in edge_copies + slot_copies + back_copies + part_copies:
        copy.wait_send()
    for copy in stores:
        copy.wait()


def on_device(tiles, groups, field, interp, conv_blocks, band_shift, owner, edge_index):
    rows, columns = field.shape
    extended, points = interp.shape
    rim = edge_index.shape[1]
    slots = conv_blocks.shape[0] * conv_blocks.shape[2]
    capacity = slots // groups
    height = rows // CHUNKS
    half, single = jnp.bfloat16, jnp.float32
    sides = pltpu.VMEM((CHUNKS, 2, height, rim), half)
    cells = pltpu.VMEM((CHUNKS, groups, height, capacity), half)
    two, many = pltpu.SemaphoreType.DMA((CHUNKS, 2)), pltpu.SemaphoreType.DMA((CHUNKS, groups))
    anywhere = pl.BlockSpec(memory_space=pl.ANY)
    return pl.pallas_call(
        functools.partial(kernel, tiles, groups),
        out_shape=jax.ShapeDtypeStruct(field.shape, single),
        in_specs=[anywhere] * 3 + [pl.BlockSpec(memory_space=pltpu.SMEM)] + [anywhere] * 2,
        out_specs=anywhere,
        scratch_shapes=[
            pltpu.VMEM(field.shape, single),
            pltpu.VMEM(interp.shape, half),
            pltpu.VMEM(conv_blocks.shape, half),
            pltpu.VMEM((1, points), jnp.int32),
            pltpu.VMEM(edge_index.shape, jnp.int32),
            pltpu.VMEM((extended, slots), half),
            pltpu.VMEM((slots, slots), half),
            pltpu.VMEM((slots, slots), half),
            pltpu.VMEM((rows, slots), single),
            pltpu.VMEM(field.shape, single),
            sides, sides, cells, cells, cells, cells, sides, sides,
            pltpu.SemaphoreType.DMA((7,)),
            pltpu.SemaphoreType.DMA((CHUNKS, 3)),
            two, two, many, many, many, many, two, two,
        ],
        compiler_params=pltpu.CompilerParams(collective_id=0, has_side_effects=True),
    )(field, interp, conv_blocks, band_shift, owner.reshape(1, points), edge_index)


def solution(mesh):
    return jax.shard_map(
        functools.partial(on_device, mesh.shape["tile"], mesh.shape["conv"]),
        mesh=mesh,
        in_specs=(
            P(None, ("tile", "conv")),
            P(("tile", "conv"), None),
            P(("tile", "conv"), None, None, None),
            P(("tile", "conv"), None),
            P(("tile", "conv"), None),
            P(("tile", "conv"), None),
        ),
        out_specs=P(None, ("tile", "conv")),
        check_vma=False,
    )
```

```python
import functools

import jax
import jax.numpy as jnp
from jax import lax
from jax.experimental import pallas as pl
from jax.experimental.pallas import tpu as pltpu
from jax.sharding import PartitionSpec as P

MESH = pl.DeviceIdType.MESH
CHUNKS = 2


def mm(left, right):
    return lax.dot_general(left, right, (((1,), (0,)), ((), ())), preferred_element_type=jnp.float32)


def mm_t(left, right):
    return lax.dot_general(left, right, (((1,), (1,)), ((), ())), preferred_element_type=jnp.float32)


def kernel(
    tiles, groups, field_hbm, interp_hbm, blocks_hbm, shift_ref, owner_hbm, edge_hbm, out_hbm,
    field, interp, blocks, owner, edge, ip, conv, gram, base, result,
    edge_out, edge_in, slot_out, slot_in, back_out, back_in, part_out, part_in,
    load_sem, store_sem, edge_send, edge_recv, slot_send, slot_recv, back_send, back_recv,
    part_send, part_recv,
):
    rows, columns = field.shape
    extended, points = interp.shape
    rim = edge.shape[1]
    owned, bands, size = blocks.shape[0], blocks.shape[1], blocks.shape[2]
    slots = owned * size
    capacity = slots // groups
    height = rows // CHUNKS
    tile, me = lax.axis_index("tile"), lax.axis_index("conv")
    count = tiles * groups
    place = tile * groups + me
    after, before = lax.rem(place + 1, count), lax.rem(place + count - 1, count)
    right = (lax.div(after, groups), lax.rem(after, groups))
    left = (lax.div(before, groups), lax.rem(before, groups))
    hops = [groups // 2] + [k for k in range(1, groups) if k != groups // 2]
    peers = [lax.rem(me + k, groups) for k in hops]

    barrier = pltpu.get_barrier_semaphore()
    for other in [left, right] + [(tile, peer) for peer in peers]:
        pl.semaphore_signal(barrier, inc=1, device_id=other, device_id_type=MESH)

    def load(source, target, index):
        copy = pltpu.make_async_copy(source, target, load_sem.at[index])
        copy.start()
        return copy

    inner = slice(rim, columns - rim)
    lead, tail = slice(0, rim), slice(columns - rim, columns)
    load_edge = load(edge_hbm, edge, 0)
    load_lead = load(field_hbm.at[:, lead], field.at[:, lead], 1)
    load_tail = load(field_hbm.at[:, tail], field.at[:, tail], 2)
    load_owner = load(owner_hbm, owner, 3)
    load_interp = load(interp_hbm, interp, 4)
    load_inner = load(field_hbm.at[:, inner], field.at[:, inner], 5)
    load_blocks = load(blocks_hbm, blocks, 6)

    def piece(chunk):
        return slice(chunk * height, (chunk + 1) * height)

    def pair(send, recv, out_ref, in_ref, chunk, side, target):
        return pltpu.make_async_remote_copy(
            src_ref=out_ref.at[chunk, side], dst_ref=in_ref.at[chunk, side],
            send_sem=send.at[chunk, side], recv_sem=recv.at[chunk, side],
            device_id=target, device_id_type=MESH,
        )

    def exchange(send, recv, out_ref, in_ref, chunk):
        copies = []
        for peer in peers:
            copies.append(pltpu.make_async_remote_copy(
                src_ref=out_ref.at[chunk, peer], dst_ref=in_ref.at[chunk, me],
                send_sem=send.at[chunk, peer], recv_sem=recv.at[chunk, me],
                device_id=(tile, peer), device_id_type=MESH,
            ))
            copies[-1].start()
        in_ref[chunk, me] = out_ref[chunk, me]
        return copies

    def arrived(send, recv, out_ref, in_ref, chunk):
        for peer in peers:
            pltpu.make_async_remote_copy(
                src_ref=out_ref.at[chunk, peer], dst_ref=in_ref.at[chunk, peer],
                send_sem=send.at[chunk, peer], recv_sem=recv.at[chunk, peer],
                device_id=(tile, peer), device_id_type=MESH,
            ).wait_recv()
        return jnp.concatenate([in_ref[chunk, g] for g in range(groups)], axis=1)

    load_edge.wait()
    lines = lax.broadcasted_iota(jnp.int32, (rim, rim), 0)
    left_pick = (lines == edge[0:1, :]).astype(jnp.float32).astype(jnp.bfloat16)
    right_pick = (lines + (columns - rim) == edge[1:2, :]).astype(jnp.float32).astype(jnp.bfloat16)
    load_lead.wait()
    load_tail.wait()
    for chunk in range(CHUNKS):
        part = piece(chunk)
        edge_out[chunk, 0] = mm(field[part, tail].astype(jnp.bfloat16), right_pick).astype(jnp.bfloat16)
        edge_out[chunk, 1] = mm(field[part, lead].astype(jnp.bfloat16), left_pick).astype(jnp.bfloat16)
    pl.semaphore_wait(barrier, 2 + len(peers))
    edge_copies, part_copies, slot_copies, back_copies = [], [], [], []
    for chunk in range(CHUNKS):
        for side, target in ((0, right), (1, left)):
            copy = pair(edge_send, edge_recv, edge_out, edge_in, chunk, side, target)
            copy.start()
            edge_copies.append(copy)

    load_owner.wait()
    owners = owner[...]
    choose = (owners == lax.broadcasted_iota(jnp.int32, (-(-groups // 8) * 8, points), 0)).astype(jnp.float32)
    order = lax.broadcasted_iota(jnp.int32, (points, points), 0) < lax.broadcasted_iota(
        jnp.int32, (points, points), 1
    )
    ranks = mm(choose.astype(jnp.bfloat16), order.astype(jnp.float32).astype(jnp.bfloat16))
    rank = jnp.sum(ranks * choose, axis=0, keepdims=True)
    slot = owners * capacity + rank.astype(jnp.int32)
    placement = (slot == lax.broadcasted_iota(jnp.int32, (slots, points), 0)).astype(jnp.float32)
    placement = placement.astype(jnp.bfloat16)
    load_interp.wait()
    ip[0:rim, :] = mm_t(interp[0:rim, :], placement).astype(jnp.bfloat16)
    ip[rim : 2 * rim, :] = mm_t(interp[extended - rim :, :], placement).astype(jnp.bfloat16)
    ip[2 * rim :, :] = mm_t(interp[rim : extended - rim, :], placement).astype(jnp.bfloat16)
    load_inner.wait()
    base[...] = mm(field[...].astype(jnp.bfloat16), ip[2 * rim :, :])

    load_blocks.wait()
    for j in range(owned):
        for s in range(owned):
            total = jnp.zeros((size, size), jnp.float32)
            for c in range(bands):
                reads = lax.rem(j + shift_ref[j, c], owned) == s
                total = total + jnp.where(reads, 1.0, 0.0) * blocks[j, c].astype(jnp.float32)
            conv[s * size : (s + 1) * size, j * size : (j + 1) * size] = total.astype(jnp.bfloat16)
    gram[...] = mm_t(conv[...], conv[...]).astype(jnp.bfloat16)

    for chunk in range(CHUNKS):
        for side, target in ((0, right), (1, left)):
            pair(edge_send, edge_recv, edge_out, edge_in, chunk, side, target).wait_recv()
        edges = jnp.concatenate([edge_in[chunk, 0], edge_in[chunk, 1]], axis=1)
        subgrid = (base[piece(chunk), :] + mm(edges, ip[0 : 2 * rim, :])).astype(jnp.bfloat16)
        for g in range(groups):
            slot_out[chunk, g] = subgrid[:, g * capacity : (g + 1) * capacity]
        slot_copies += exchange(slot_send, slot_recv, slot_out, slot_in, chunk)

    for chunk in range(CHUNKS):
        gathered = arrived(slot_send, slot_recv, slot_out, slot_in, chunk)
        adjoint = mm(gathered, gram[...]).astype(jnp.bfloat16)
        for g in range(groups):
            back_out[chunk, g] = adjoint[:, g * capacity : (g + 1) * capacity]
        back_copies += exchange(back_send, back_recv, back_out, back_in, chunk)

    stores = []
    for chunk in range(CHUNKS):
        part = piece(chunk)
        returned = arrived(back_send, back_recv, back_out, back_in, chunk)
        rims = mm_t(returned, ip[0 : 2 * rim, :]).astype(jnp.bfloat16)
        part_out[chunk, 0] = rims[:, rim:]
        part_out[chunk, 1] = rims[:, :rim]
        for side, target in ((0, right), (1, left)):
            copy = pair(part_send, part_recv, part_out, part_in, chunk, side, target)
            copy.start()
            part_copies.append(copy)
        result[part, :] = mm_t(returned, ip[2 * rim :, :])
        copy = pltpu.make_async_copy(
            result.at[part, inner], out_hbm.at[part, inner], store_sem.at[chunk, 0]
        )
        copy.start()
        stores.append(copy)

    for chunk in range(CHUNKS):
        part = piece(chunk)
        for side, where, pick, target in ((0, lead, left_pick, right), (1, tail, right_pick, left)):
            pair(part_send, part_recv, part_out, part_in, chunk, side, target).wait_recv()
            result[part, where] += mm_t(part_in[chunk, side], pick)
            copy = pltpu.make_async_copy(
                result.at[part, where], out_hbm.at[part, where], store_sem.at[chunk, 1 + side]
            )
            copy.start()
            stores.append(copy)
    for copy in edge_copies + slot_copies + back_copies + part_copies:
        copy.wait_send()
    for copy in stores:
        copy.wait()


def on_device(tiles, groups, field, interp, conv_blocks, band_shift, owner, edge_index):
    rows, columns = field.shape
    extended, points = interp.shape
    rim = edge_index.shape[1]
    slots = conv_blocks.shape[0] * conv_blocks.shape[2]
    capacity = slots // groups
    height = rows // CHUNKS
    half, single = jnp.bfloat16, jnp.float32
    sides = pltpu.VMEM((CHUNKS, 2, height, rim), half)
    cells = pltpu.VMEM((CHUNKS, groups, height, capacity), half)
    two, many = pltpu.SemaphoreType.DMA((CHUNKS, 2)), pltpu.SemaphoreType.DMA((CHUNKS, groups))
    anywhere = pl.BlockSpec(memory_space=pl.ANY)
    return pl.pallas_call(
        functools.partial(kernel, tiles, groups),
        out_shape=jax.ShapeDtypeStruct(field.shape, single),
        in_specs=[anywhere] * 3 + [pl.BlockSpec(memory_space=pltpu.SMEM)] + [anywhere] * 2,
        out_specs=anywhere,
        scratch_shapes=[
            pltpu.VMEM(field.shape, single),
            pltpu.VMEM(interp.shape, half),
            pltpu.VMEM(conv_blocks.shape, half),
            pltpu.VMEM((1, points), jnp.int32),
            pltpu.VMEM(edge_index.shape, jnp.int32),
            pltpu.VMEM((extended, slots), half),
            pltpu.VMEM((slots, slots), half),
            pltpu.VMEM((slots, slots), half),
            pltpu.VMEM((rows, slots), single),
            pltpu.VMEM(field.shape, single),
            sides, sides, cells, cells, cells, cells, sides, sides,
            pltpu.SemaphoreType.DMA((7,)),
            pltpu.SemaphoreType.DMA((CHUNKS, 3)),
            two, two, many, many, many, many, two, two,
        ],
        compiler_params=pltpu.CompilerParams(collective_id=0, has_side_effects=True),
    )(field, interp, conv_blocks, band_shift, owner.reshape(1, points), edge_index)


def solution(mesh):
    return jax.shard_map(
        functools.partial(on_device, mesh.shape["tile"], mesh.shape["conv"]),
        mesh=mesh,
        in_specs=(
            P(None, ("tile", "conv")),
            P(("tile", "conv"), None),
            P(("tile", "conv"), None, None, None),
            P(("tile", "conv"), None),
            P(("tile", "conv"), None),
            P(("tile", "conv"), None),
        ),
        out_specs=P(None, ("tile", "conv")),
        check_vma=False,
    )
```

```python
import functools

import jax
import jax.numpy as jnp
from jax import lax
from jax.experimental import pallas as pl
from jax.experimental.pallas import tpu as pltpu
from jax.sharding import PartitionSpec as P

MESH = pl.DeviceIdType.MESH
CHUNKS = 2


def mm(left, right):
    return lax.dot_general(left, right, (((1,), (0,)), ((), ())), preferred_element_type=jnp.float32)


def mm_t(left, right):
    return lax.dot_general(left, right, (((1,), (1,)), ((), ())), preferred_element_type=jnp.float32)


def kernel(
    tiles, groups, rim, field_hbm, interp_hbm, blocks_hbm, lists, result,
    field, interp, blocks, ip, conv, gram, base,
    edge_out, edge_in, slot_out, slot_in, back_out, back_in, part_out, part_in,
    load_sem, edge_send, edge_recv, slot_send, slot_recv, back_send, back_recv,
    part_send, part_recv,
):
    rows, columns = field.shape
    extended, points = interp.shape
    owned, bands, size = blocks.shape[0], blocks.shape[1], blocks.shape[2]
    slots = owned * size
    capacity = slots // groups
    height = rows // CHUNKS
    tile, me = lax.axis_index("tile"), lax.axis_index("conv")
    count = tiles * groups
    place = tile * groups + me
    after, before = lax.rem(place + 1, count), lax.rem(place + count - 1, count)
    right = (lax.div(after, groups), lax.rem(after, groups))
    left = (lax.div(before, groups), lax.rem(before, groups))
    hops = [groups // 2] + [k for k in range(1, groups) if k != groups // 2]
    peers = [lax.rem(me + k, groups) for k in hops]

    barrier = pltpu.get_barrier_semaphore()
    for other in [left, right] + [(tile, peer) for peer in peers]:
        pl.semaphore_signal(barrier, inc=1, device_id=other, device_id_type=MESH)

    def load(source, target, index):
        copy = pltpu.make_async_copy(source, target, load_sem.at[index])
        copy.start()
        return copy

    inner = slice(rim, columns - rim)
    lead, tail = slice(0, rim), slice(columns - rim, columns)
    load_lead = load(field_hbm.at[:, lead], field.at[:, lead], 1)
    load_tail = load(field_hbm.at[:, tail], field.at[:, tail], 2)
    load_interp = load(interp_hbm, interp, 4)
    load_inner = load(field_hbm.at[:, inner], field.at[:, inner], 5)
    load_blocks = load(blocks_hbm, blocks, 6)

    def piece(chunk):
        return slice(chunk * height, (chunk + 1) * height)

    def pair(send, recv, out_ref, in_ref, chunk, side, target):
        return pltpu.make_async_remote_copy(
            src_ref=out_ref.at[chunk, side], dst_ref=in_ref.at[chunk, side],
            send_sem=send.at[chunk, side], recv_sem=recv.at[chunk, side],
            device_id=target, device_id_type=MESH,
        )

    def exchange(send, recv, out_ref, in_ref, chunk):
        copies = []
        for peer in peers:
            copies.append(pltpu.make_async_remote_copy(
                src_ref=out_ref.at[chunk, peer], dst_ref=in_ref.at[chunk, me],
                send_sem=send.at[chunk, peer], recv_sem=recv.at[chunk, me],
                device_id=(tile, peer), device_id_type=MESH,
            ))
            copies[-1].start()
        in_ref[chunk, me] = out_ref[chunk, me]
        return copies

    def arrived(send, recv, out_ref, in_ref, chunk):
        for peer in peers:
            pltpu.make_async_remote_copy(
                src_ref=out_ref.at[chunk, peer], dst_ref=in_ref.at[chunk, peer],
                send_sem=send.at[chunk, peer], recv_sem=recv.at[chunk, peer],
                device_id=(tile, peer), device_id_type=MESH,
            ).wait_recv()
        return jnp.concatenate([in_ref[chunk, g] for g in range(groups)], axis=1)

    left_list = lists[:, points : points + rim]
    right_list = lists[:, points + rim : points + 2 * rim]
    lines = lax.broadcasted_iota(jnp.int32, (rim, rim), 0)
    left_pick = (lines == left_list).astype(jnp.float32).astype(jnp.bfloat16)
    right_pick = (lines + (columns - rim) == right_list).astype(jnp.float32).astype(jnp.bfloat16)
    load_lead.wait()
    load_tail.wait()
    for chunk in range(CHUNKS):
        part = piece(chunk)
        edge_out[chunk, 0] = mm(field[part, tail].astype(jnp.bfloat16), right_pick).astype(jnp.bfloat16)
        edge_out[chunk, 1] = mm(field[part, lead].astype(jnp.bfloat16), left_pick).astype(jnp.bfloat16)
    pl.semaphore_wait(barrier, 2 + len(peers))
    edge_copies, part_copies, slot_copies, back_copies = [], [], [], []
    for chunk in range(CHUNKS):
        for side, target in ((0, right), (1, left)):
            copy = pair(edge_send, edge_recv, edge_out, edge_in, chunk, side, target)
            copy.start()
            edge_copies.append(copy)

    owners = lists[:, 0:points]
    choose = (owners == lax.broadcasted_iota(jnp.int32, (-(-groups // 8) * 8, points), 0)).astype(jnp.float32)
    order = lax.broadcasted_iota(jnp.int32, (points, points), 0) < lax.broadcasted_iota(
        jnp.int32, (points, points), 1
    )
    ranks = mm(choose.astype(jnp.bfloat16), order.astype(jnp.float32).astype(jnp.bfloat16))
    rank = jnp.sum(ranks * choose, axis=0, keepdims=True)
    slot = owners * capacity + rank.astype(jnp.int32)
    placement = (slot == lax.broadcasted_iota(jnp.int32, (slots, points), 0)).astype(jnp.float32)
    placement = placement.astype(jnp.bfloat16)
    load_interp.wait()
    ip[0:rim, :] = mm_t(interp[0:rim, :], placement).astype(jnp.bfloat16)
    ip[rim : 2 * rim, :] = mm_t(interp[extended - rim :, :], placement).astype(jnp.bfloat16)
    ip[2 * rim :, :] = mm_t(interp[rim : extended - rim, :], placement).astype(jnp.bfloat16)
    load_inner.wait()
    base[...] = mm(field[...].astype(jnp.bfloat16), ip[2 * rim :, :])

    load_blocks.wait()
    for j in range(owned):
        for s in range(owned):
            total = jnp.zeros((size, size), jnp.float32)
            for c in range(bands):
                at = points + 2 * rim + j * bands + c
                reads = lax.rem(j + lists[:, at : at + 1], owned) == s
                total = total + jnp.where(reads, 1.0, 0.0) * blocks[j, c].astype(jnp.float32)
            conv[s * size : (s + 1) * size, j * size : (j + 1) * size] = total.astype(jnp.bfloat16)
    gram[...] = mm_t(conv[...], conv[...]).astype(jnp.bfloat16)

    for chunk in range(CHUNKS):
        for side, target in ((0, right), (1, left)):
            pair(edge_send, edge_recv, edge_out, edge_in, chunk, side, target).wait_recv()
        edges = jnp.concatenate([edge_in[chunk, 0], edge_in[chunk, 1]], axis=1)
        subgrid = (base[piece(chunk), :] + mm(edges, ip[0 : 2 * rim, :])).astype(jnp.bfloat16)
        for g in range(groups):
            slot_out[chunk, g] = subgrid[:, g * capacity : (g + 1) * capacity]
        slot_copies += exchange(slot_send, slot_recv, slot_out, slot_in, chunk)

    for chunk in range(CHUNKS):
        gathered = arrived(slot_send, slot_recv, slot_out, slot_in, chunk)
        adjoint = mm(gathered, gram[...]).astype(jnp.bfloat16)
        for g in range(groups):
            back_out[chunk, g] = adjoint[:, g * capacity : (g + 1) * capacity]
        back_copies += exchange(back_send, back_recv, back_out, back_in, chunk)

    for chunk in range(CHUNKS):
        part = piece(chunk)
        returned = arrived(back_send, back_recv, back_out, back_in, chunk)
        rims = mm_t(returned, ip[0 : 2 * rim, :]).astype(jnp.bfloat16)
        part_out[chunk, 0] = rims[:, rim:]
        part_out[chunk, 1] = rims[:, :rim]
        for side, target in ((0, right), (1, left)):
            copy = pair(part_send, part_recv, part_out, part_in, chunk, side, target)
            copy.start()
            part_copies.append(copy)
        result[part, :] = mm_t(returned, ip[2 * rim :, :])

    for chunk in range(CHUNKS):
        part = piece(chunk)
        for side, where, pick, target in ((0, lead, left_pick, right), (1, tail, right_pick, left)):
            pair(part_send, part_recv, part_out, part_in, chunk, side, target).wait_recv()
            result[part, where] += mm_t(part_in[chunk, side], pick)
    for copy in edge_copies + slot_copies + back_copies + part_copies:
        copy.wait_send()


def on_device(tiles, groups, field, interp, conv_blocks, band_shift, owner, edge_index):
    rows, columns = field.shape
    extended, points = interp.shape
    rim = edge_index.shape[1]
    slots = conv_blocks.shape[0] * conv_blocks.shape[2]
    capacity = slots // groups
    height = rows // CHUNKS
    half, single = jnp.bfloat16, jnp.float32
    sides = pltpu.VMEM((CHUNKS, 2, height, rim), half)
    cells = pltpu.VMEM((CHUNKS, groups, height, capacity), half)
    two, many = pltpu.SemaphoreType.DMA((CHUNKS, 2)), pltpu.SemaphoreType.DMA((CHUNKS, groups))
    lists = jnp.concatenate([owner.reshape(-1), edge_index.reshape(-1), band_shift.reshape(-1)])
    lists = jnp.pad(lists, (0, -lists.size % 128)).reshape(1, -1)
    anywhere = pl.BlockSpec(memory_space=pl.ANY)
    return pl.pallas_call(
        functools.partial(kernel, tiles, groups, rim),
        out_shape=jax.ShapeDtypeStruct(field.shape, single),
        in_specs=[anywhere] * 3 + [pl.BlockSpec(memory_space=pltpu.VMEM)],
        out_specs=pl.BlockSpec(memory_space=pltpu.VMEM),
        scratch_shapes=[
            pltpu.VMEM(field.shape, single),
            pltpu.VMEM(interp.shape, half),
            pltpu.VMEM(conv_blocks.shape, half),
            pltpu.VMEM((extended, slots), half),
            pltpu.VMEM((slots, slots), half),
            pltpu.VMEM((slots, slots), half),
            pltpu.VMEM((rows, slots), single),
            sides, sides, cells, cells, cells, cells, sides, sides,
            pltpu.SemaphoreType.DMA((7,)),
            two, two, many, many, many, many, two, two,
        ],
        compiler_params=pltpu.CompilerParams(collective_id=0, has_side_effects=True, vmem_limit_bytes=53 * 2**20),
    )(field, interp, conv_blocks, lists)


def solution(mesh):
    return jax.shard_map(
        functools.partial(on_device, mesh.shape["tile"], mesh.shape["conv"]),
        mesh=mesh,
        in_specs=(
            P(None, ("tile", "conv")),
            P(("tile", "conv"), None),
            P(("tile", "conv"), None, None, None),
            P(("tile", "conv"), None),
            P(("tile", "conv"), None),
            P(("tile", "conv"), None),
        ),
        out_specs=P(None, ("tile", "conv")),
        check_vma=False,
    )
```
